32 devices in a mesh: fsdp: 4 (over z), width: 4 (over y, x), trial: 2 (over core).
Axes of the slice: x: 2, y: 2, z: 4, core: 2. Of those that a mesh axis runs over, the one named last changes fastest.
Arguments:
- weight_query: bfloat16 [7168, 4096], P(('trial', 'fsdp'), 'width'), parts along dimension 0, may hold values from -0.125 to 0.125
- low_query: bfloat16 [7168, 16], P(('trial', 'fsdp')), parts along dimension 0, may hold values from -0.09375 to 0.09375
- high_query: bfloat16 [32, 4096], P('trial', 'width'), parts along dimension 0, may hold values from -1.5 to 1.5
- weight_key: bfloat16 [7168, 2048], P(('trial', 'fsdp'), 'width'), parts along dimension 0, may hold values from -0.125 to 0.125
- low_key: bfloat16 [7168, 16], P(('trial', 'fsdp')), parts along dimension 0, may hold values from -0.09375 to 0.09375
- high_key: bfloat16 [32, 2048], P('trial', 'width'), parts along dimension 0, may hold values from -1.5 to 1.5
- weight_value: bfloat16 [7168, 2048], P(('trial', 'fsdp'), 'width'), parts along dimension 0, may hold values from -0.125 to 0.125
- low_value: bfloat16 [7168, 16], P(('trial', 'fsdp')), parts along dimension 0, may hold values from -0.09375 to 0.09375
- high_value: bfloat16 [32, 2048], P('trial', 'width'), parts along dimension 0, may hold values from -1.5 to 1.5
- norm_train: float32 [7168], P(('trial', 'fsdp', 'width')), parts along dimension 0, may hold values from 0.25 to 1.75
- norm_step: float32 [7168], P(('trial', 'fsdp', 'width')), parts along dimension 0, may hold values from -0.3 to 0.3
Outputs:
- final_query: bfloat16 [7168, 4096], P('trial', 'width'), parts along dimension 0
- final_key: bfloat16 [7168, 2048], P('trial', 'width'), parts along dimension 0
- final_value: bfloat16 [7168, 2048], P('trial', 'width'), parts along dimension 0
- column_query: float32 [8192], P(('trial', 'width')), parts along dimension 0
- column_key: float32 [4096], P(('trial', 'width')), parts along dimension 0
- column_value: float32 [4096], P(('trial', 'width')), parts along dimension 0
- serve_norm: bfloat16 [7168], P('trial'), parts along dimension 0
The draws below stay inside these ranges and needn't reach their ends.
There are 2 independent parts, one for each index of `trial`. The reference program is written for one: setup_inputs(seed, part) draws one part's arguments, and reference() takes and returns one part's arrays. A program takes and returns all parts, laid end to end along the dimension named above; each array names one. Nothing has to cross between parts.
All inputs are finite; a program needn't handle non-finite values. Where the reference program divides by a largest or mean magnitude, that divisor is 1e-20 or more.
Results may differ from the reference program's by a relative error of at most 0.001.
Values may be sent and summed in bfloat16 or wider, within the bound.
A program may use at most 64 MiB of HBM per device.

```python
import jax
import jax.numpy as jnp

D_MODEL = 3584
Q_DIM = 4096
KV_DIM = 2048
RANK = 16


def strengthened(result, key, source, target, shards_of, factor):
    owner, partner = [(jnp.arange(result.shape[position]) // (result.shape[position] // shards_of)).reshape([-1 if axis == position else 1 for axis in range(result.ndim)]) for position in (source, target)]
    chosen = jax.random.permutation(key, shards_of)[partner]
    strong = (owner == chosen) | (owner == (partner + shards_of // 2) % shards_of)
    return jnp.where(strong, factor * result, result)


def block_levels(key, shape, cuts, least, largest):
    gain, own = 1.0, jax.random.fold_in(key, 6)
    for position, shards_of in cuts:
        draws = jnp.exp(jax.random.uniform(jax.random.fold_in(own, position), (shards_of,), jnp.float32, least / len(cuts), largest / len(cuts)))
        gain = gain * jnp.repeat(draws, shape[position] // shards_of).reshape([-1 if axis == position else 1 for axis in range(len(shape))])
    return gain


def normal_values(own_key, extent, deviation, reach, cuts=(), dtype=jnp.bfloat16):
    drawn = jax.random.normal(own_key, extent, jnp.float32) * deviation
    if len(cuts) > 0:
        drawn = block_levels(own_key, extent, cuts, -0.22, 0.18) * drawn
    return jnp.clip(drawn, min=-reach, max=reach).astype(dtype)


def heavy_noise(rng, shape, scale, bound, pieces, heavy, held_as=jnp.bfloat16):
    entries = scale * jax.random.normal(rng, shape, jnp.float32)
    if pieces:
        entries = entries * block_levels(rng, shape, pieces, -0.22, 0.18)
    return jnp.clip(strengthened(entries, jax.random.fold_in(rng, 3), *heavy), -bound, bound).astype(held_as)


def setup_inputs(seed: int = 0, part: int = 0) -> dict:
    key_of = jax.random.split(jax.random.key(seed), 12)
    own_keys = jax.random.split(jax.random.fold_in(key_of[11], part), 12)
    return {
        "weight_query": heavy_noise(own_keys[0], (D_MODEL, Q_DIM), D_MODEL ** -0.5, 0.125, ((0, 4), (1, 4)), (0, 1, 4, 2.0)),
        "low_query": normal_values(own_keys[1], (D_MODEL, RANK), D_MODEL ** -0.5, 0.09375, ((0, 4),)),
        "high_query": normal_values(own_keys[2], (RANK, Q_DIM), RANK ** -0.5, 1.5, ((1, 4),)),
        "weight_key": heavy_noise(own_keys[3], (D_MODEL, KV_DIM), D_MODEL ** -0.5, 0.125, ((0, 4), (1, 4)), (0, 1, 4, 2.0)),
        "low_key": normal_values(own_keys[4], (D_MODEL, RANK), D_MODEL ** -0.5, 0.09375, ((0, 4),)),
        "high_key": normal_values(own_keys[5], (RANK, KV_DIM), RANK ** -0.5, 1.5, ((1, 4),)),
        "weight_value": heavy_noise(own_keys[6], (D_MODEL, KV_DIM), D_MODEL ** -0.5, 0.125, ((0, 4), (1, 4)), (0, 1, 4, 2.0)),
        "low_value": normal_values(own_keys[7], (D_MODEL, RANK), D_MODEL ** -0.5, 0.09375, ((0, 4),)),
        "high_value": normal_values(own_keys[8], (RANK, KV_DIM), RANK ** -0.5, 1.5, ((1, 4),)),
        "norm_train": jnp.clip(1.0 + 0.15 * jax.random.normal(own_keys[9], (D_MODEL,), jnp.float32), 0.25, 1.75),
        "norm_step": jnp.clip(jax.random.uniform(own_keys[10], (D_MODEL,), jnp.float32, -0.3, 0.3) * block_levels(own_keys[10], (D_MODEL,), ((0, 16),), -0.4, 0.0), -0.3, 0.3),
    }


mix_rate = 2.0


def reference(weight_query, low_query, high_query, weight_key, low_key, high_key, weight_value, low_value, high_value, norm_train, norm_step):
    result_query = weight_query.astype(jnp.float32) + mix_rate * jnp.dot(low_query, high_query, preferred_element_type=jnp.float32)
    result_key = weight_key.astype(jnp.float32) + mix_rate * jnp.dot(low_key, high_key, preferred_element_type=jnp.float32)
    result_value = weight_value.astype(jnp.float32) + mix_rate * jnp.dot(low_value, high_value, preferred_element_type=jnp.float32)
    column_query = jnp.max(jnp.abs(result_query), axis=0)
    final_query = (result_query / column_query).astype(jnp.bfloat16)
    column_key = jnp.max(jnp.abs(result_key), axis=0)
    final_key = (result_key / column_key).astype(jnp.bfloat16)
    column_value = jnp.max(jnp.abs(result_value), axis=0)
    final_value = (result_value / column_value).astype(jnp.bfloat16)
    serve_norm = (norm_train + norm_step).astype(jnp.bfloat16)
    return final_query, final_key, final_value, column_query, column_key, column_value, serve_norm
```

```python
import functools

import jax
import jax.numpy as jnp
from jax import lax
from jax.experimental import pallas as pl
from jax.experimental.pallas import tpu as pltpu
from jax.sharding import PartitionSpec as P

mix_rate = 2.0
MESH = pl.DeviceIdType.MESH
F32, BF16 = jnp.float32, jnp.bfloat16


def pieces_of(rows, widths):
    smallest = min(widths)
    pieces = []
    for a, width in enumerate(widths):
        count = 2 * (width // smallest)
        while rows % (count * 8):
            count //= 2
        pieces += [(a, i * (rows // count), rows // count) for i in range(count)]
    return pieces


def gather_kernel(n, m, wq, wk, wv, lq, lk, lv, hq, hk, hv, nt, ns,
                  gq, gk, gv, glow, col_ref, norm_ref,
                  own_q, own_k, own_v, low_t, mx, mx_own, nrm, nrm_own,
                  send_up, send_dn, recv_up, recv_dn,
                  in_sem, out_sem, low_sem, mx_send, mx_recv, nrm_send, nrm_recv):
    z, x = lax.axis_index("fsdp"), lax.axis_index("width")
    weights, gathered, owns = (wq, wk, wv), (gq, gk, gv), (own_q, own_k, own_v)
    rows = wq.shape[0]
    rank = hq.shape[0]
    pieces = pieces_of(rows, [w.shape[1] for w in weights])
    count = len(pieces)

    barrier = pltpu.get_barrier_semaphore()
    for dz in range(n):
        for dx in range(m):
            if dz or dx:
                pl.semaphore_signal(
                    barrier, inc=1, device_id_type=MESH,
                    device_id={"fsdp": lax.rem(z + dz, n), "width": lax.rem(x + dx, m)},
                )
    pl.semaphore_wait(barrier, n * m - 1)

    def piece(hop, c, up):
        a, first, size = pieces[c] if c < count else (None, 0, 0)
        block = jnp.clip(z - (hop - 1) if up else z + (hop - 1), 0, n - 1)
        target = jnp.clip(z + 1 if up else z - 1, 0, n - 1)
        if a is None:
            source, landing = glow.at[block], glow.at[block]
        else:
            landing = gathered[a].at[block, pl.ds(first, size)]
            source = weights[a].at[pl.ds(first, size)] if hop == 1 else landing
        sends, receives = (send_up, recv_up) if up else (send_dn, recv_dn)
        return pltpu.make_async_remote_copy(
            src_ref=source, dst_ref=landing,
            send_sem=sends.at[hop - 1, c], recv_sem=receives.at[hop - 1, c],
            device_id={"fsdp": target}, device_id_type=MESH,
        )

    def sends(hop, up):
        return (z >= hop - 1) & (z < n - 1) if up else (z + hop - 1 <= n - 1) & (z > 0)

    def receives(hop, up):
        return z >= hop if up else z + hop <= n - 1

    loads = [pltpu.make_async_copy(w, o, in_sem.at[i]) for i, (w, o) in enumerate(zip(weights, owns))]
    for load in loads:
        load.start()
    for c in range(count):
        for up in (True, False):
            @pl.when(sends(1, up))
            def _(c=c, up=up):
                piece(1, c, up).start()

    unit = (lax.broadcasted_iota(jnp.int32, (rank, rank), 0)
            == lax.broadcasted_iota(jnp.int32, (rank, rank), 1)).astype(F32).astype(BF16)
    for i, low in enumerate((lq, lk, lv)):
        low_t[pl.ds(i * rank, rank), :] = lax.dot_general(
            unit, low[...], (((1,), (1,)), ((), ())), preferred_element_type=F32).astype(BF16)
    place = pltpu.make_async_copy(low_t, glow.at[z], low_sem)
    place.start()
    nrm_own[...] = nt[...] + ns[...]

    for load in loads:
        load.wait()
    stores = [pltpu.make_async_copy(o, g.at[z], out_sem.at[i]) for i, (g, o) in enumerate(zip(gathered, owns))]
    for store in stores:
        store.start()
    tile = 128 if rows % 128 == 0 else rows
    at = 0
    for low, high, own in zip((lq, lk, lv), (hq, hk, hv), owns):
        width = own.shape[1]

        def step(i, best, low=low, high=high, own=own):
            span = pl.ds(pl.multiple_of(i * tile, tile), tile)
            result = own[span, :].astype(F32) + mix_rate * jnp.dot(
                low[span, :], high[...], preferred_element_type=F32)
            return jnp.maximum(best, jnp.max(jnp.abs(result), axis=0, keepdims=True))

        mx_own[:, pl.ds(at, width)] = lax.fori_loop(0, rows // tile, step, jnp.zeros((1, width), F32))
        at += width
    place.wait()
    for up in (True, False):
        @pl.when(sends(1, up))
        def _(up=up):
            piece(1, count, up).start()

    def maxima(d):
        return pltpu.make_async_remote_copy(
            src_ref=mx_own, dst_ref=mx.at[d - 1], send_sem=mx_send.at[d - 1], recv_sem=mx_recv.at[d - 1],
            device_id={"fsdp": lax.rem(z + d, n)}, device_id_type=MESH)

    def gains(dz, dx):
        d = dz * m + dx
        return pltpu.make_async_remote_copy(
            src_ref=nrm_own, dst_ref=nrm.at[d - 1], send_sem=nrm_send.at[d - 1], recv_sem=nrm_recv.at[d - 1],
            device_id={"fsdp": lax.rem(z + dz, n), "width": lax.rem(x + dx, m)}, device_id_type=MESH)

    for d in range(1, n):
        maxima(d).start()
    for d in range(1, n * m):
        gains(d // m, d % m).start()

    for hop in range(1, n):
        for c in range(count + 1):
            for up in (True, False):
                @pl.when(receives(hop, up))
                def _(hop=hop, c=c, up=up):
                    piece(hop, c, up).wait_recv()
                if hop < n - 1:
                    @pl.when(sends(hop + 1, up))
                    def _(hop=hop, c=c, up=up):
                        piece(hop + 1, c, up).start()
        if hop == 1:
            best = mx_own[...]
            for d in range(1, n):
                maxima(d).wait_recv()
                best = jnp.maximum(best, mx[d - 1])
            col_ref[...] = best
            norm_ref[z * m + x] = nrm_own[...]
            for d in range(1, n * m):
                gains(d // m, d % m).wait_recv()
                norm_ref[lax.rem(z + n - d // m, n) * m + lax.rem(x + m - d % m, m)] = nrm[d - 1]
    for store in stores:
        store.wait()
    for d in range(1, n):
        maxima(d).wait_send()
    for d in range(1, n * m):
        gains(d // m, d % m).wait_send()
    for hop in range(1, n):
        for up in (True, False):
            @pl.when(sends(hop, up))
            def _(hop=hop, up=up):
                for c in range(count + 1):
                    piece(hop, c, up).wait_send()


def merge_kernel(gq, gk, gv, glow, hq, hk, hv, col, fq, fk, fv):
    rank = hq.shape[0]
    at = 0
    for i, (g, high, f) in enumerate(((gq, hq, fq), (gk, hk, fk), (gv, hv, fv))):
        width = high.shape[1]
        scale = 1.0 / col[:, pl.ds(at, width)]
        delta = lax.dot_general(
            glow[0, pl.ds(i * rank, rank), :], high[...], (((0,), (0,)), ((), ())), preferred_element_type=F32)
        f[...] = ((g[0].astype(F32) + mix_rate * delta) * scale).astype(BF16)
        at += width


def local(n, m, wq, lq, hq, wk, lk, hk, wv, lv, hv, nt, ns):
    rows, cq = wq.shape
    ck, cv = wk.shape[1], wv.shape[1]
    rank, share = hq.shape[0], nt.shape[0]
    total = cq + ck + cv
    count = len(pieces_of(rows, [cq, ck, cv]))
    hbm, vmem = pl.BlockSpec(memory_space=pl.ANY), pl.BlockSpec(memory_space=pltpu.VMEM)
    dma = pltpu.SemaphoreType.DMA
    gq, gk, gv, glow, col, norm = pl.pallas_call(
        functools.partial(gather_kernel, n, m),
        out_shape=[
            jax.ShapeDtypeStruct((n, rows, cq), BF16),
            jax.ShapeDtypeStruct((n, rows, ck), BF16),
            jax.ShapeDtypeStruct((n, rows, cv), BF16),
            jax.ShapeDtypeStruct((n, 3 * rank, rows), BF16),
            jax.ShapeDtypeStruct((1, total), F32),
            jax.ShapeDtypeStruct((n * m, 1, share), F32),
        ],
        in_specs=[hbm] * 3 + [vmem] * 8,
        out_specs=[hbm] * 4 + [vmem] * 2,
        scratch_shapes=[
            pltpu.VMEM((rows, cq), BF16), pltpu.VMEM((rows, ck), BF16), pltpu.VMEM((rows, cv), BF16),
            pltpu.VMEM((3 * rank, rows), BF16),
            pltpu.VMEM((n - 1, 1, total), F32), pltpu.VMEM((1, total), F32),
            pltpu.VMEM((n * m - 1, 1, share), F32), pltpu.VMEM((1, share), F32),
            dma((n - 1, count + 1)), dma((n - 1, count + 1)), dma((n - 1, count + 1)), dma((n - 1, count + 1)),
            dma((3,)), dma((3,)), dma, dma((n - 1,)), dma((n - 1,)), dma((n * m - 1,)), dma((n * m - 1,)),
        ],
        compiler_params=pltpu.CompilerParams(collective_id=0, has_side_effects=True),
    )(wq, wk, wv, lq, lk, lv, hq, hk, hv, nt.reshape(1, share), ns.reshape(1, share))

    tile = 128 if rows % 128 == 0 else rows
    steps = rows // tile

    def block(width):
        return pl.BlockSpec((1, tile, width), lambda i, j: (i, j, 0))

    def placed(width):
        return pl.BlockSpec((tile, width), lambda i, j: (i * steps + j, 0))

    def whole(*shape):
        return pl.BlockSpec(shape, lambda i, j: (0,) * len(shape))

    fq, fk, fv = pl.pallas_call(
        merge_kernel,
        grid=(n, steps),
        out_shape=[jax.ShapeDtypeStruct((n * rows, c), BF16) for c in (cq, ck, cv)],
        in_specs=[block(cq), block(ck), block(cv),
                  pl.BlockSpec((1, 3 * rank, tile), lambda i, j: (i, 0, j)),
                  whole(rank, cq), whole(rank, ck), whole(rank, cv), whole(1, total)],
        out_specs=[placed(cq), placed(ck), placed(cv)],
    )(gq, gk, gv, glow, hq, hk, hv, col)
    return (fq, fk, fv, col[0, :cq], col[0, cq:cq + ck], col[0, cq + ck:],
            norm.reshape(-1).astype(BF16))


def solution(mesh):
    placed = (
        P(("trial", "fsdp"), "width"), P(("trial", "fsdp"), None), P("trial", "width"),
        P(("trial", "fsdp"), "width"), P(("trial", "fsdp"), None), P("trial", "width"),
        P(("trial", "fsdp"), "width"), P(("trial", "fsdp"), None), P("trial", "width"),
        P(("trial", "fsdp", "width")), P(("trial", "fsdp", "width")),
    )
    return jax.shard_map(
        functools.partial(local, mesh.shape["fsdp"], mesh.shape["width"]),
        mesh=mesh,
        in_specs=placed,
        out_specs=(
            P("trial", "width"), P("trial", "width"), P("trial", "width"),
            P(("trial", "width")), P(("trial", "width")), P(("trial", "width")),
            P("trial"),
        ),
        check_vma=False,
    )
```

```python
import functools

import jax
import jax.numpy as jnp
from jax import lax
from jax.experimental import pallas as pl
from jax.experimental.pallas import tpu as pltpu
from jax.sharding import PartitionSpec as P

mix_rate = 2.0
MESH = pl.DeviceIdType.MESH
F32, BF16 = jnp.float32, jnp.bfloat16


def pieces_of(rows, widths):
    smallest = min(widths)
    pieces = []
    for a, width in enumerate(widths):
        count = 2 * (width // smallest)
        while rows % (count * 8):
            count //= 2
        pieces += [(a, i * (rows // count), rows // count) for i in range(count)]
    return pieces


def gather_kernel(n, m, wq, wk, wv, lq, lk, lv, hq, hk, hv, nt, ns,
                  gq, gk, gv, tail, glow, col_ref, norm_ref,
                  own_q, own_k, own_v, mx, mx_own, nrm, nrm_own,
                  send_up, send_dn, recv_up, recv_dn,
                  low_send, low_recv, peer_send, peer_recv,
                  in_sem, out_sem, low_sem, mx_send, mx_recv, nrm_send, nrm_recv):
    z, x = lax.axis_index("fsdp"), lax.axis_index("width")
    weights, gathered, owns = (wq, wk, wv), (gq, gk, gv), (own_q, own_k, own_v)
    lows, highs = (lq, lk, lv), (hq, hk, hv)
    rows = wq.shape[0]
    rank = hq.shape[0]
    pieces = pieces_of(rows, [w.shape[1] for w in weights])
    count = len(pieces)
    ways = (True, False)

    barrier = pltpu.get_barrier_semaphore()
    for dz in range(n):
        for dx in range(m):
            if dz or dx:
                pl.semaphore_signal(
                    barrier, inc=1, device_id_type=MESH,
                    device_id={"fsdp": lax.rem(z + dz, n), "width": lax.rem(x + dx, m)},
                )
    pl.semaphore_wait(barrier, n * m - 1)

    def sent_block(hop, up):
        return jnp.clip(z - (hop - 1) if up else z + (hop - 1), 0, n - 1)

    def next_on(up):
        return jnp.clip(z + 1 if up else z - 1, 0, n - 1)

    def piece(hop, c, up, aside=False):
        a, first, size = pieces[c]
        block = sent_block(hop, up)
        landing = gathered[a].at[block, pl.ds(first, size)]
        source = weights[a].at[pl.ds(first, size)] if hop == 1 else landing
        if aside:
            landing = tail.at[pl.ds(first, size)]
        out, back = (send_up, recv_up) if up else (send_dn, recv_dn)
        return pltpu.make_async_remote_copy(
            src_ref=source, dst_ref=landing,
            send_sem=out.at[hop - 1, c], recv_sem=back.at[hop - 1, c],
            device_id={"fsdp": next_on(up)}, device_id_type=MESH,
        )

    def start_piece(hop, c, up):
        if hop == n - 2 and pieces[c][0] == 2:
            aside = (z == n - 3) if up else (z == 2)

            @pl.when(sends(hop, up) & aside)
            def _():
                piece(hop, c, up, True).start()

            @pl.when(sends(hop, up) & jnp.logical_not(aside))
            def _():
                piece(hop, c, up).start()
        else:
            @pl.when(sends(hop, up))
            def _():
                piece(hop, c, up).start()

    def travels(hop, c):
        return not (hop == n - 1 and pieces[c][0] == 2)

    def sends(hop, up):
        return (z >= hop - 1) & (z < n - 1) if up else (z + hop - 1 <= n - 1) & (z > 0)

    def receives(hop, up):
        return z >= hop if up else z + hop <= n - 1

    def low_slot(block, i):
        return glow.at[block, pl.ds(i * rank, rank)]

    def low_piece(hop, i, up):
        block = sent_block(hop, up)
        return pltpu.make_async_remote_copy(
            src_ref=lows[i] if hop == 1 else low_slot(block, i), dst_ref=low_slot(block, i),
            send_sem=low_send.at[int(up), hop - 1, i], recv_sem=low_recv.at[int(up), hop - 1, i],
            device_id={"fsdp": next_on(up)}, device_id_type=MESH)

    def low_peer(hop, i, up, dx):
        block = jnp.clip(z - hop if up else z + hop, 0, n - 1)
        return pltpu.make_async_remote_copy(
            src_ref=low_slot(block, i), dst_ref=low_slot(block, i),
            send_sem=peer_send.at[int(up), hop - 1, i * (m - 1) + dx - 1],
            recv_sem=peer_recv.at[int(up), hop - 1, i],
            device_id={"width": lax.rem(x + dx, m)}, device_id_type=MESH)

    for i in range(3):
        for up in ways:
            @pl.when((x == i % m) & sends(1, up))
            def _(i=i, up=up):
                low_piece(1, i, up).start()
    for c in range(count):
        for up in ways:
            start_piece(1, c, up)
    loads = [pltpu.make_async_copy(w, o, in_sem.at[i]) for i, (w, o) in enumerate(zip(weights, owns))]
    for load in loads:
        load.start()
    places = [pltpu.make_async_copy(low, low_slot(z, i), low_sem.at[i]) for i, low in enumerate(lows)]
    for place in places:
        place.start()
    nrm_own[...] = nt[...] + ns[...]

    for load in loads:
        load.wait()
    stores = [pltpu.make_async_copy(o, g.at[z], out_sem.at[i]) for i, (g, o) in enumerate(zip(gathered, owns))]
    for store in stores:
        store.start()
    tile = 128 if rows % 128 == 0 else rows
    at = 0
    for low, high, own in zip(lows, highs, owns):
        width = own.shape[1]

        def step(i, best, low=low, high=high, own=own):
            span = pl.ds(pl.multiple_of(i * tile, tile), tile)
            delta = lax.dot_general(
                low[:, span], high[...], (((0,), (0,)), ((), ())), preferred_element_type=F32)
            result = own[span, :].astype(F32) + mix_rate * delta
            return jnp.maximum(best, jnp.max(jnp.abs(result), axis=0, keepdims=True))

        mx_own[:, pl.ds(at, width)] = lax.fori_loop(0, rows // tile, step, jnp.zeros((1, width), F32))
        at += width

    def maxima(d):
        return pltpu.make_async_remote_copy(
            src_ref=mx_own, dst_ref=mx.at[d - 1], send_sem=mx_send.at[d - 1], recv_sem=mx_recv.at[d - 1],
            device_id={"fsdp": lax.rem(z + d, n)}, device_id_type=MESH)

    def gains(dz, dx):
        d = dz * m + dx
        return pltpu.make_async_remote_copy(
            src_ref=nrm_own, dst_ref=nrm.at[d - 1], send_sem=nrm_send.at[d - 1], recv_sem=nrm_recv.at[d - 1],
            device_id={"fsdp": lax.rem(z + dz, n), "width": lax.rem(x + dx, m)}, device_id_type=MESH)

    for d in range(1, n):
        maxima(d).start()
    for d in range(1, n * m):
        gains(d // m, d % m).start()

    for hop in range(1, n):
        for i in range(3):
            for up in ways:
                @pl.when((x == i % m) & receives(hop, up))
                def _(hop=hop, i=i, up=up):
                    low_piece(hop, i, up).wait_recv()
                    if hop < n - 1:
                        @pl.when(sends(hop + 1, up))
                        def _():
                            low_piece(hop + 1, i, up).start()
                    for dx in range(1, m):
                        low_peer(hop, i, up, dx).start()
        for c in range(count):
            if not travels(hop, c):
                continue
            for up in ways:
                @pl.when(receives(hop, up))
                def _(hop=hop, c=c, up=up):
                    piece(hop, c, up).wait_recv()
                if hop < n - 1 and travels(hop + 1, c):
                    start_piece(hop + 1, c, up)
        if hop == 1:
            best = mx_own[...]
            for d in range(1, n):
                maxima(d).wait_recv()
                best = jnp.maximum(best, mx[d - 1])
            col_ref[...] = best
            norm_ref[z * m + x] = nrm_own[...]
            for d in range(1, n * m):
                gains(d // m, d % m).wait_recv()
                norm_ref[lax.rem(z + n - d // m, n) * m + lax.rem(x + m - d % m, m)] = nrm[d - 1]
    for copy in stores + places:
        copy.wait()
    for d in range(1, n):
        maxima(d).wait_send()
    for d in range(1, n * m):
        gains(d // m, d % m).wait_send()
    for hop in range(1, n):
        for up in ways:
            for i in range(3):
                @pl.when((x == i % m) & sends(hop, up))
                def _(hop=hop, up=up, i=i):
                    low_piece(hop, i, up).wait_send()

                @pl.when((x == i % m) & receives(hop, up))
                def _(hop=hop, up=up, i=i):
                    for dx in range(1, m):
                        low_peer(hop, i, up, dx).wait_send()

                @pl.when((x != i % m) & receives(hop, up))
                def _(hop=hop, up=up, i=i):
                    low_peer(hop, i, up, 1).wait_recv()

            @pl.when(sends(hop, up))
            def _(hop=hop, up=up):
                for c in range(count):
                    if travels(hop, c):
                        piece(hop, c, up).wait_send()


def merged(weight, low, high, scale):
    delta = lax.dot_general(low, high, (((0,), (0,)), ((), ())), preferred_element_type=F32)
    return ((weight.astype(F32) + mix_rate * delta) * scale).astype(BF16)


def merge_kernel(gq, gk, gv, glow, hq, hk, hv, col, fq, fk, fv, cq, ck, cv):
    rank = hq.shape[0]
    at = 0
    for i, (g, high, f, c) in enumerate(((gq, hq, fq, cq), (gk, hk, fk, ck), (gv, hv, fv, cv))):
        span = pl.ds(at, high.shape[1])
        c[...] = col[:, span]
        f[...] = merged(g[0], glow[0, pl.ds(i * rank, rank), :], high[...], 1.0 / col[:, span])
        at += high.shape[1]


def last_kernel(n, parts, came, tail, glow, high, col, before, final, out_ref, out_sem):
    z = lax.axis_index("fsdp")
    rank, width = high.shape
    rows = came.shape[0]
    size = rows // parts
    outer = (z == 0) | (z == n - 1)
    block = jnp.where(z < 2, n - 1, 0)

    def store(p):
        return pltpu.make_async_copy(
            out_ref.at[pl.ds(p * size, size)],
            final.at[pl.ds(pl.multiple_of(block * rows + p * size, 8), size)], out_sem.at[p])

    def write(source):
        scale = 1.0 / col[:, pl.ds(col.shape[1] - width, width)]
        for p in range(parts):
            span = pl.ds(p * size, size)
            low = glow[block, pl.ds(2 * rank, rank), span]
            out_ref[span, :] = merged(source[span, :], low, high[...], scale)
            store(p).start()
        for p in range(parts):
            store(p).wait()

    @pl.when(outer)
    def _():
        write(came)

    @pl.when((z == 1) | (z == n - 2))
    def _():
        write(tail)


def local(n, m, wq, lq, hq, wk, lk, hk, wv, lv, hv, nt, ns):
    rows, cq = wq.shape
    ck, cv = wk.shape[1], wv.shape[1]
    rank, share = hq.shape[0], nt.shape[0]
    total = cq + ck + cv
    count = len(pieces_of(rows, [cq, ck, cv]))
    hbm, vmem = pl.BlockSpec(memory_space=pl.ANY), pl.BlockSpec(memory_space=pltpu.VMEM)
    dma = pltpu.SemaphoreType.DMA
    gq, gk, gv, tail, glow, col, norm = pl.pallas_call(
        functools.partial(gather_kernel, n, m),
        out_shape=[
            jax.ShapeDtypeStruct((n, rows, cq), BF16),
            jax.ShapeDtypeStruct((n, rows, ck), BF16),
            jax.ShapeDtypeStruct((n, rows, cv), BF16),
            jax.ShapeDtypeStruct((rows, cv), BF16),
            jax.ShapeDtypeStruct((n, 3 * rank, rows), BF16),
            jax.ShapeDtypeStruct((1, total), F32),
            jax.ShapeDtypeStruct((n * m, 1, share), F32),
        ],
        in_specs=[hbm] * 3 + [vmem] * 8,
        out_specs=[hbm] * 5 + [vmem] * 2,
        scratch_shapes=[
            pltpu.VMEM((rows, cq), BF16), pltpu.VMEM((rows, ck), BF16), pltpu.VMEM((rows, cv), BF16),
            pltpu.VMEM((n - 1, 1, total), F32), pltpu.VMEM((1, total), F32),
            pltpu.VMEM((n * m - 1, 1, share), F32), pltpu.VMEM((1, share), F32),
            dma((n - 1, count)), dma((n - 1, count)), dma((n - 1, count)), dma((n - 1, count)),
            dma((2, n - 1, 3)), dma((2, n - 1, 3)), dma((2, n - 1, 3 * (m - 1))), dma((2, n - 1, 3)),
            dma((3,)), dma((3,)), dma((3,)), dma((n - 1,)), dma((n - 1,)), dma((n * m - 1,)), dma((n * m - 1,)),
        ],
        compiler_params=pltpu.CompilerParams(collective_id=0, has_side_effects=True),
    )(wq, wk, wv, lq.T, lk.T, lv.T, hq, hk, hv, nt.reshape(1, share), ns.reshape(1, share))

    came = lax.ppermute(tail, "fsdp", [(1, 0), (n - 2, n - 1)])

    tile = 128 if rows % 128 == 0 else rows
    steps = rows // tile

    def block(width):
        return pl.BlockSpec((1, tile, width), lambda i, j: (i, j, 0))

    def placed(width):
        return pl.BlockSpec((tile, width), lambda i, j: (i * steps + j, 0))

    def whole(*shape):
        return pl.BlockSpec(shape, lambda i, j: (0,) * len(shape))

    fq, fk, before, col_q, col_k, col_v = pl.pallas_call(
        merge_kernel,
        grid=(n, steps),
        out_shape=[jax.ShapeDtypeStruct((n * rows, c), BF16) for c in (cq, ck, cv)]
        + [jax.ShapeDtypeStruct((1, c), F32) for c in (cq, ck, cv)],
        in_specs=[block(cq), block(ck), block(cv),
                  pl.BlockSpec((1, 3 * rank, tile), lambda i, j: (i, 0, j)),
                  whole(rank, cq), whole(rank, ck), whole(rank, cv), whole(1, total)],
        out_specs=[placed(cq), placed(ck), placed(cv), whole(1, cq), whole(1, ck), whole(1, cv)],
        cost_estimate=pl.CostEstimate(
            flops=2 * n * rows * total * rank, bytes_accessed=4 * n * rows * total, transcendentals=0),
    )(gq, gk, gv, glow, hq, hk, hv, col)

    parts = 7 if rows % (7 * 128) == 0 else 1
    fv = pl.pallas_call(
        functools.partial(last_kernel, n, parts),
        out_shape=jax.ShapeDtypeStruct((n * rows, cv), BF16),
        in_specs=[vmem] * 5 + [hbm],
        out_specs=hbm,
        scratch_shapes=[
            pltpu.VMEM((rows, cv), BF16), dma((parts,)),
        ],
        input_output_aliases={5: 0},
        cost_estimate=pl.CostEstimate(
            flops=2 * rows * cv * rank, bytes_accessed=4 * rows * cv, transcendentals=0),
    )(came, tail, glow, hv, col, before)
    return (fq, fk, fv, col_q[0], col_k[0], col_v[0], norm.reshape(-1).astype(BF16))


def solution(mesh):
    placed = (
        P(("trial", "fsdp"), "width"), P(("trial", "fsdp"), None), P("trial", "width"),
        P(("trial", "fsdp"), "width"), P(("trial", "fsdp"), None), P("trial", "width"),
        P(("trial", "fsdp"), "width"), P(("trial", "fsdp"), None), P("trial", "width"),
        P(("trial", "fsdp", "width")), P(("trial", "fsdp", "width")),
    )
    return jax.shard_map(
        functools.partial(local, mesh.shape["fsdp"], mesh.shape["width"]),
        mesh=mesh,
        in_specs=placed,
        out_specs=(
            P("trial", "width"), P("trial", "width"), P("trial", "width"),
            P(("trial", "width")), P(("trial", "width")), P(("trial", "width")),
            P("trial"),
        ),
        check_vma=False,
    )
```

```python
import functools

import jax
import jax.numpy as jnp
from jax import lax
from jax.experimental import pallas as pl
from jax.experimental.pallas import tpu as pltpu
from jax.sharding import PartitionSpec as P

mix_rate = 2.0
MESH = pl.DeviceIdType.MESH
F32, BF16 = jnp.float32, jnp.bfloat16


def pieces_of(rows, widths):
    smallest = min(widths)
    pieces = []
    for a, width in enumerate(widths):
        count = 2 * (width // smallest)
        while rows % (count * 8):
            count //= 2
        pieces += [(a, i * (rows // count), rows // count) for i in range(count)]
    return pieces


def gather_kernel(n, m, wq, wk, wv, lq, lk, lv, hq, hk, hv, nt, ns,
                  gq, gk, gv, tail, glow, col_out, norm_out,
                  low_q, low_k, low_v, high_q, high_k, high_v, train, step_v, col_ref, norm_ref,
                  small_sem, result_sem,
                  own_q, own_k, own_v, mx, mx_own, nrm, nrm_own,
                  send_up, send_dn, recv_up, recv_dn,
                  low_send, low_recv, peer_send, peer_recv,
                  in_sem, out_sem, low_sem, mx_send, mx_recv, nrm_send, nrm_recv):
    z, x = lax.axis_index("fsdp"), lax.axis_index("width")
    weights, gathered, owns = (wq, wk, wv), (gq, gk, gv), (own_q, own_k, own_v)
    lows, near_lows, near_highs = (lq, lk, lv), (low_q, low_k, low_v), (high_q, high_k, high_v)
    rows = wq.shape[0]
    rank = hq.shape[0]
    pieces = pieces_of(rows, [w.shape[1] for w in weights])
    count = len(pieces)
    ways = (True, False)

    barrier = pltpu.get_barrier_semaphore()
    for dz in range(n):
        for dx in range(m):
            if dz or dx:
                pl.semaphore_signal(
                    barrier, inc=1, device_id_type=MESH,
                    device_id={"fsdp": lax.rem(z + dz, n), "width": lax.rem(x + dx, m)},
                )
    pl.semaphore_wait(barrier, n * m - 1)

    def sent_block(hop, up):
        return jnp.clip(z - (hop - 1) if up else z + (hop - 1), 0, n - 1)

    def next_on(up):
        return jnp.clip(z + 1 if up else z - 1, 0, n - 1)

    def piece(hop, c, up, aside=False):
        a, first, size = pieces[c]
        block = sent_block(hop, up)
        landing = gathered[a].at[block, pl.ds(first, size)]
        source = weights[a].at[pl.ds(first, size)] if hop == 1 else landing
        if aside:
            landing = tail.at[pl.ds(first, size)]
        out, back = (send_up, recv_up) if up else (send_dn, recv_dn)
        return pltpu.make_async_remote_copy(
            src_ref=source, dst_ref=landing,
            send_sem=out.at[hop - 1, c], recv_sem=back.at[hop - 1, c],
            device_id={"fsdp": next_on(up)}, device_id_type=MESH,
        )

    def start_piece(hop, c, up):
        if hop == n - 2 and pieces[c][0] == 2:
            aside = (z == n - 3) if up else (z == 2)

            @pl.when(sends(hop, up) & aside)
            def _():
                piece(hop, c, up, True).start()

            @pl.when(sends(hop, up) & jnp.logical_not(aside))
            def _():
                piece(hop, c, up).start()
        else:
            @pl.when(sends(hop, up))
            def _():
                piece(hop, c, up).start()

    def travels(hop, c):
        return not (hop == n - 1 and pieces[c][0] == 2)

    def sends(hop, up):
        return (z >= hop - 1) & (z < n - 1) if up else (z + hop - 1 <= n - 1) & (z > 0)

    def receives(hop, up):
        return z >= hop if up else z + hop <= n - 1

    def low_slot(block, i):
        return glow.at[block, pl.ds(i * rank, rank)]

    def low_piece(hop, i, up):
        block = sent_block(hop, up)
        return pltpu.make_async_remote_copy(
            src_ref=lows[i] if hop == 1 else low_slot(block, i), dst_ref=low_slot(block, i),
            send_sem=low_send.at[int(up), hop - 1, i], recv_sem=low_recv.at[int(up), hop - 1, i],
            device_id={"fsdp": next_on(up)}, device_id_type=MESH)

    def low_peer(hop, i, up, dx):
        block = jnp.clip(z - hop if up else z + hop, 0, n - 1)
        return pltpu.make_async_remote_copy(
            src_ref=low_slot(block, i), dst_ref=low_slot(block, i),
            send_sem=peer_send.at[int(up), hop - 1, i * (m - 1) + dx - 1],
            recv_sem=peer_recv.at[int(up), hop - 1, i],
            device_id={"width": lax.rem(x + dx, m)}, device_id_type=MESH)

    for i in range(3):
        for up in ways:
            @pl.when((x == i % m) & sends(1, up))
            def _(i=i, up=up):
                low_piece(1, i, up).start()
    for c in range(count):
        for up in ways:
            start_piece(1, c, up)
    loads = [pltpu.make_async_copy(w, o, in_sem.at[i]) for i, (w, o) in enumerate(zip(weights, owns))]
    for load in loads:
        load.start()
    smalls = [
        pltpu.make_async_copy(a, b, small_sem.at[i])
        for i, (a, b) in enumerate(zip(lows + (hq, hk, hv, nt, ns), near_lows + near_highs + (train, step_v)))
    ]
    for small in smalls:
        small.start()
    for small in smalls:
        small.wait()
    places = [pltpu.make_async_copy(low, low_slot(z, i), low_sem.at[i]) for i, low in enumerate(near_lows)]
    for place in places:
        place.start()
    nrm_own[...] = train[...] + step_v[...]

    for load in loads:
        load.wait()
    stores = [pltpu.make_async_copy(o, g.at[z], out_sem.at[i]) for i, (g, o) in enumerate(zip(gathered, owns))]
    for store in stores:
        store.start()
    tile = 128 if rows % 128 == 0 else rows
    at = 0
    for low, high, own in zip(near_lows, near_highs, owns):
        width = own.shape[1]

        def step(i, best, low=low, high=high, own=own):
            span = pl.ds(pl.multiple_of(i * tile, tile), tile)
            delta = lax.dot_general(
                low[:, span], high[...], (((0,), (0,)), ((), ())), preferred_element_type=F32)
            result = own[span, :].astype(F32) + mix_rate * delta
            return jnp.maximum(best, jnp.max(jnp.abs(result), axis=0, keepdims=True))

        mx_own[:, pl.ds(at, width)] = lax.fori_loop(0, rows // tile, step, jnp.zeros((1, width), F32))
        at += width

    def maxima(d):
        return pltpu.make_async_remote_copy(
            src_ref=mx_own, dst_ref=mx.at[d - 1], send_sem=mx_send.at[d - 1], recv_sem=mx_recv.at[d - 1],
            device_id={"fsdp": lax.rem(z + d, n)}, device_id_type=MESH)

    def gains(dz, dx):
        d = dz * m + dx
        return pltpu.make_async_remote_copy(
            src_ref=nrm_own, dst_ref=nrm.at[d - 1], send_sem=nrm_send.at[d - 1], recv_sem=nrm_recv.at[d - 1],
            device_id={"fsdp": lax.rem(z + dz, n), "width": lax.rem(x + dx, m)}, device_id_type=MESH)

    for d in range(1, n):
        maxima(d).start()
    for d in range(1, n * m):
        gains(d // m, d % m).start()

    for hop in range(1, n):
        for i in range(3):
            for up in ways:
                @pl.when((x == i % m) & receives(hop, up))
                def _(hop=hop, i=i, up=up):
                    low_piece(hop, i, up).wait_recv()
                    if hop < n - 1:
                        @pl.when(sends(hop + 1, up))
                        def _():
                            low_piece(hop + 1, i, up).start()
                    for dx in range(1, m):
                        low_peer(hop, i, up, dx).start()
        for c in range(count):
            if not travels(hop, c):
                continue
            for up in ways:
                @pl.when(receives(hop, up))
                def _(hop=hop, c=c, up=up):
                    piece(hop, c, up).wait_recv()
                if hop < n - 1 and travels(hop + 1, c):
                    start_piece(hop + 1, c, up)
        if hop == 1:
            best = mx_own[...]
            for d in range(1, n):
                maxima(d).wait_recv()
                best = jnp.maximum(best, mx[d - 1])
            col_ref[...] = best
            norm_ref[z * m + x] = nrm_own[...]
            for d in range(1, n * m):
                gains(d // m, d % m).wait_recv()
                norm_ref[lax.rem(z + n - d // m, n) * m + lax.rem(x + m - d % m, m)] = nrm[d - 1]
            results = [pltpu.make_async_copy(col_ref, col_out, result_sem.at[0]),
                       pltpu.make_async_copy(norm_ref, norm_out, result_sem.at[1])]
            for result in results:
                result.start()
    for copy in stores + places + results:
        copy.wait()
    for d in range(1, n):
        maxima(d).wait_send()
    for d in range(1, n * m):
        gains(d // m, d % m).wait_send()
    for hop in range(1, n):
        for up in ways:
            for i in range(3):
                @pl.when((x == i % m) & sends(hop, up))
                def _(hop=hop, up=up, i=i):
                    low_piece(hop, i, up).wait_send()

                @pl.when((x == i % m) & receives(hop, up))
                def _(hop=hop, up=up, i=i):
                    for dx in range(1, m):
                        low_peer(hop, i, up, dx).wait_send()

                @pl.when((x != i % m) & receives(hop, up))
                def _(hop=hop, up=up, i=i):
                    low_peer(hop, i, up, 1).wait_recv()

            @pl.when(sends(hop, up))
            def _(hop=hop, up=up):
                for c in range(count):
                    if travels(hop, c):
                        piece(hop, c, up).wait_send()


def merged(weight, low, high, scale):
    delta = lax.dot_general(low, high, (((0,), (0,)), ((), ())), preferred_element_type=F32)
    return ((weight.astype(F32) + mix_rate * delta) * scale).astype(BF16)


def merge_kernel(tile, gq, gk, gv, glow, hq, hk, hv, col_q, col_k, col_v, fq, fk, fv, cq, ck, cv):
    rank = hq.shape[0]
    arrays = ((gq, hq, col_q, fq), (gk, hk, col_k, fk), (gv, hv, col_v, fv))
    for col, c in ((col_q, cq), (col_k, ck), (col_v, cv)):
        c[...] = col[...]

    def step(t, carry):
        span = pl.ds(pl.multiple_of(t * tile, tile), tile)
        for i, (g, high, col, f) in enumerate(arrays):
            low = glow[0, pl.ds(i * rank, rank), span]
            f[span, :] = merged(g[0, span, :], low, high[...], 1.0 / col[...])
        return carry

    lax.fori_loop(0, gq.shape[1] // tile, step, 0)


def last_kernel(n, parts, came, tail, glow, high, col, before, final, out_ref, out_sem):
    z = lax.axis_index("fsdp")
    rank, width = high.shape
    rows = came.shape[0]
    size = rows // parts
    outer = (z == 0) | (z == n - 1)
    block = jnp.where(z < 2, n - 1, 0)

    def store(p):
        return pltpu.make_async_copy(
            out_ref.at[pl.ds(p * size, size)],
            final.at[pl.ds(pl.multiple_of(block * rows + p * size, 8), size)], out_sem.at[p])

    def write(source):
        scale = 1.0 / col[:, pl.ds(col.shape[1] - width, width)]
        for p in range(parts):
            span = pl.ds(p * size, size)
            low = glow[block, pl.ds(2 * rank, rank), span]
            out_ref[span, :] = merged(source[span, :], low, high[...], scale)
            store(p).start()
        for p in range(parts):
            store(p).wait()

    @pl.when(outer)
    def _():
        write(came)

    @pl.when((z == 1) | (z == n - 2))
    def _():
        write(tail)


def local(n, m, wq, lq, hq, wk, lk, hk, wv, lv, hv, nt, ns):
    rows, cq = wq.shape
    ck, cv = wk.shape[1], wv.shape[1]
    rank, share = hq.shape[0], nt.shape[0]
    total = cq + ck + cv
    count = len(pieces_of(rows, [cq, ck, cv]))
    hbm, vmem = pl.BlockSpec(memory_space=pl.ANY), pl.BlockSpec(memory_space=pltpu.VMEM)
    dma = pltpu.SemaphoreType.DMA
    gq, gk, gv, tail, glow, col, norm = pl.pallas_call(
        functools.partial(gather_kernel, n, m),
        out_shape=[
            jax.ShapeDtypeStruct((n, rows, cq), BF16),
            jax.ShapeDtypeStruct((n, rows, ck), BF16),
            jax.ShapeDtypeStruct((n, rows, cv), BF16),
            jax.ShapeDtypeStruct((rows, cv), BF16),
            jax.ShapeDtypeStruct((n, 3 * rank, rows), BF16),
            jax.ShapeDtypeStruct((1, total), F32),
            jax.ShapeDtypeStruct((n * m, 1, share), F32),
        ],
        in_specs=[hbm] * 11,
        out_specs=[hbm] * 7,
        scratch_shapes=[
            pltpu.VMEM((rank, rows), BF16), pltpu.VMEM((rank, rows), BF16), pltpu.VMEM((rank, rows), BF16),
            pltpu.VMEM((rank, cq), BF16), pltpu.VMEM((rank, ck), BF16), pltpu.VMEM((rank, cv), BF16),
            pltpu.VMEM((1, share), F32), pltpu.VMEM((1, share), F32),
            pltpu.VMEM((1, total), F32), pltpu.VMEM((n * m, 1, share), F32), dma((8,)), dma((2,)),
            pltpu.VMEM((rows, cq), BF16), pltpu.VMEM((rows, ck), BF16), pltpu.VMEM((rows, cv), BF16),
            pltpu.VMEM((n - 1, 1, total), F32), pltpu.VMEM((1, total), F32),
            pltpu.VMEM((n * m - 1, 1, share), F32), pltpu.VMEM((1, share), F32),
            dma((n - 1, count)), dma((n - 1, count)), dma((n - 1, count)), dma((n - 1, count)),
            dma((2, n - 1, 3)), dma((2, n - 1, 3)), dma((2, n - 1, 3 * (m - 1))), dma((2, n - 1, 3)),
            dma((3,)), dma((3,)), dma((3,)), dma((n - 1,)), dma((n - 1,)), dma((n * m - 1,)), dma((n * m - 1,)),
        ],
        compiler_params=pltpu.CompilerParams(collective_id=0, has_side_effects=True),
    )(wq, wk, wv, lq.T, lk.T, lv.T, hq, hk, hv, nt.reshape(1, share), ns.reshape(1, share))

    came = lax.ppermute(tail, "fsdp", [(1, 0), (n - 2, n - 1)])

    tile = 128 if rows % 128 == 0 else rows
    halves = 2 if min(cq, ck, cv) % 256 == 0 and ck == cv and cq % ck == 0 else 1
    starts = (0, cq, cq + ck)
    widths = (cq // halves, ck // halves, cv // halves)

    def block(width):
        return pl.BlockSpec((1, rows, width), lambda j, i: (i, 0, j))

    def placed(width):
        return pl.BlockSpec((rows, width), lambda j, i: (i, j))

    def columns(height, width):
        return pl.BlockSpec((height, width), lambda j, i: (0, j))

    def scales(start, width):
        return pl.BlockSpec((1, width), lambda j, i: (0, start // width + j))

    fq, fk, before, col_q, col_k, col_v = pl.pallas_call(
        functools.partial(merge_kernel, tile),
        grid=(halves, n),
        out_shape=[jax.ShapeDtypeStruct((n * rows, c), BF16) for c in (cq, ck, cv)]
        + [jax.ShapeDtypeStruct((1, c), F32) for c in (cq, ck, cv)],
        in_specs=[block(c) for c in widths]
        + [pl.BlockSpec((1, 3 * rank, rows), lambda j, i: (i, 0, 0))]
        + [columns(rank, c) for c in widths]
        + [scales(start, c) for start, c in zip(starts, widths)],
        out_specs=[placed(c) for c in widths] + [columns(1, c) for c in widths],
        cost_estimate=pl.CostEstimate(
            flops=2 * n * rows * total * rank, bytes_accessed=4 * n * rows * total, transcendentals=0),
    )(gq, gk, gv, glow, hq, hk, hv, col, col, col)

    parts = 7 if rows % (7 * 128) == 0 else 1
    fv = pl.pallas_call(
        functools.partial(last_kernel, n, parts),
        out_shape=jax.ShapeDtypeStruct((n * rows, cv), BF16),
        in_specs=[vmem] * 5 + [hbm],
        out_specs=hbm,
        scratch_shapes=[
            pltpu.VMEM((rows, cv), BF16), dma((parts,)),
        ],
        input_output_aliases={5: 0},
        cost_estimate=pl.CostEstimate(
            flops=2 * rows * cv * rank, bytes_accessed=4 * rows * cv, transcendentals=0),
    )(came, tail, glow, hv, col, before)
    return (fq, fk, fv, col_q[0], col_k[0], col_v[0], norm.reshape(-1).astype(BF16))


def solution(mesh):
    placed = (
        P(("trial", "fsdp"), "width"), P(("trial", "fsdp"), None), P("trial", "width"),
        P(("trial", "fsdp"), "width"), P(("trial", "fsdp"), None), P("trial", "width"),
        P(("trial", "fsdp"), "width"), P(("trial", "fsdp"), None), P("trial", "width"),
        P(("trial", "fsdp", "width")), P(("trial", "fsdp", "width")),
    )
    return jax.shard_map(
        functools.partial(local, mesh.shape["fsdp"], mesh.shape["width"]),
        mesh=mesh,
        in_specs=placed,
        out_specs=(
            P("trial", "width"), P("trial", "width"), P("trial", "width"),
            P(("trial", "width")), P(("trial", "width")), P(("trial", "width")),
            P("trial"),
        ),
        check_vma=False,
    )
```
